32 devices in a mesh: cp: 4 (over z), tp: 8 (over y, x, core).
Axes of the slice: x: 2, y: 2, z: 4, core: 2. Of those that a mesh axis runs over, the one named last changes fastest.
Arguments:
- checkpoint: bfloat16 [2048, 8192], P('cp', 'tp'), may hold values from -6 to 6
- norm_gain: float32 [8192], replicated, may hold values from 0.1 to 1.9
- query_weight: bfloat16 [8192, 8192], P(None, 'tp'), may hold values from -4 to 4
- key_weight: bfloat16 [8192, 1024], P(None, 'tp'), may hold values from -1 to 1
- value_weight: bfloat16 [8192, 1024], P(None, 'tp'), may hold values from -0.0625 to 0.0625
- output_weight: bfloat16 [8192, 8192], P('tp'), may hold values from -0.09375 to 0.09375
- block_order: int32 [8], replicated, may hold values from 0 to 7, each once
Outputs:
- projected: bfloat16 [2048, 8192], P('cp', 'tp')
- log_normalizer: float32 [64, 2048], P('tp', 'cp')
The draws below stay inside these ranges and needn't reach their ends.
Inputs may be any that keep to these rules, and one draw needn't show every extreme that they name: `block_order`: each of 0 to 7 once.
All inputs are finite; a program needn't handle non-finite values.
Results may differ from the reference program's by a relative error of at most 0.019.
Values may be sent and summed in bfloat16 or wider, within the bound.
No kernel may reach another device: no remote copies, remote signals or barrier semaphores. Data moves between devices by JAX's collectives and lax.ppermute only.
A program may use at most 128 MiB of HBM per device.

```python
import math
import jax
import jax.numpy as jnp
from jax import lax

D = 8192
HEADS = 64
KV_HEADS = 8
HEAD_DIM = 128
SEQ = 2048
BLOCK = 256
N_CP = 4
N_TP = 8


def joint_query_key(key):
    shared_keys = jax.random.normal(jax.random.fold_in(key, 17), (D, KV_HEADS * HEAD_DIM), jnp.float32) / math.sqrt(D)
    shared_keys = jnp.clip(shared_keys, -1.0, 1.0)
    queries = jax.random.normal(jax.random.fold_in(key, 29), (D, HEADS * HEAD_DIM), jnp.float32) * (2.5 / math.sqrt(D))
    queries = jnp.clip(queries, -4.0, 4.0)
    return (queries, shared_keys)


def draw_query_weight(key, part):
    return joint_query_key(key)[0].astype(jnp.bfloat16)


def draw_key_weight(key, part):
    return joint_query_key(key)[1].astype(jnp.bfloat16)


def raised(values, stream_key, source, target, parts, factor):
    def block_of(axis_at):
        return (jnp.arange(values.shape[axis_at]) // (values.shape[axis_at] // parts)).reshape((-1,) + (1,) * (values.ndim - 1 - axis_at))

    first = jax.random.permutation(stream_key, parts)[block_of(target)]
    second = (block_of(target) + parts // 2) % parts
    return jnp.where((block_of(source) == first) | (block_of(source) == second), factor * values, values)


def steps_of(rng, dims, cuts, smallest, largest):
    def one(dim, blocks):
        steps = jax.random.uniform(jax.random.fold_in(jax.random.fold_in(rng, 6), dim), (blocks,), jnp.float32, smallest / len(cuts), largest / len(cuts))
        return jnp.repeat(jnp.exp(steps), dims[dim] // blocks).reshape((-1,) + (1,) * (len(dims) - dim - 1))

    gain = one(*cuts[0])
    for cut in cuts[1:]:
        gain = gain * one(*cut)
    return gain


def scatter_about(own_key, dims, spread, limit, shards=(), held_as=jnp.bfloat16):
    result = spread * jax.random.normal(own_key, dims, jnp.float32)
    if shards:
        result = result * steps_of(own_key, dims, shards, -0.22, 0.18)
    return jnp.clip(result, -limit, limit).astype(held_as)


def heavy_noise(own_key, shape, spread, limit, cuts, heavy, kind=jnp.bfloat16):
    entries = spread * jax.random.normal(own_key, shape, jnp.float32)
    if cuts:
        entries = entries * steps_of(own_key, shape, cuts, -0.22, 0.18)
    return jnp.clip(raised(entries, jax.random.fold_in(own_key, 3), *heavy), -limit, limit).astype(kind)


def setup_inputs(seed: int = 0) -> dict:
    streams_of = jax.random.split(jax.random.key(seed), 8)
    checkpoint = scatter_about(streams_of[0], (SEQ, D), 1.0, 6.0, ((0, 4), (1, 8)))
    norm_gain = jnp.clip(1.0 + 0.18 * jax.random.normal(streams_of[1], (D,), jnp.float32), 0.1, 1.9)
    query_weight = draw_query_weight(jax.random.fold_in(streams_of[7], 71), 0)
    key_weight = draw_key_weight(jax.random.fold_in(streams_of[7], 71), 0)
    value_weight = scatter_about(streams_of[4], (D, KV_HEADS * HEAD_DIM), D ** -0.5, 0.0625, ((1, 8),))
    output_weight = heavy_noise(streams_of[5], (HEADS * HEAD_DIM, D), (HEADS * HEAD_DIM) ** -0.5, 0.09375, ((0, 8),), (0, 1, 8, 2.0))
    block_order = jax.random.permutation(streams_of[6], 2 * N_CP).astype(jnp.int32)
    return {"checkpoint": checkpoint, "norm_gain": norm_gain, "query_weight": query_weight, "key_weight": key_weight, "value_weight": value_weight, "output_weight": output_weight, "block_order": block_order}


rope_base = 500000.0
norm_epsilon = 1e-05

def turn_pairs(matrix, positions, first_pair):
    pair_count = matrix.shape[-1] // 2
    pair_index = (first_pair + jnp.arange(pair_count, dtype=jnp.int32)).astype(jnp.float32)
    inverse_rates = rope_base ** (-2.0 * pair_index / HEAD_DIM)
    angles = positions.astype(jnp.float32)[:, None] * inverse_rates[None, :]
    cosine = jnp.cos(angles)[:, None, :]
    sine_part = jnp.sin(angles)[:, None, :]
    paired = matrix.reshape(matrix.shape[0], matrix.shape[1], pair_count, 2)
    former = paired[..., 0]
    latter = paired[..., 1]
    turned = jnp.stack([former * cosine - latter * sine_part, former * sine_part + latter * cosine], axis=-1)
    return turned.reshape(matrix.shape)

def reference(checkpoint, norm_gain, query_weight, key_weight, value_weight, output_weight, block_order):
    seq_rows = jnp.arange(SEQ, dtype=jnp.int32)
    positions = (block_order[seq_rows // BLOCK] * BLOCK + seq_rows % BLOCK).astype(jnp.int32)
    widened = checkpoint.astype(jnp.float32)
    mean_square = lax.optimization_barrier(jnp.mean(widened * widened, axis=-1, keepdims=True))
    normed = (widened * lax.rsqrt(mean_square + norm_epsilon) * norm_gain).astype(jnp.bfloat16)
    query_features = jnp.dot(normed, query_weight, preferred_element_type=jnp.float32)
    key_features = jnp.dot(normed, key_weight, preferred_element_type=jnp.float32)
    value_features = jnp.dot(normed, value_weight, preferred_element_type=jnp.float32)
    queries = turn_pairs(query_features.reshape(SEQ, HEADS, HEAD_DIM), positions, 0).astype(jnp.bfloat16)
    keys = turn_pairs(key_features.reshape(SEQ, KV_HEADS, HEAD_DIM), positions, 0).astype(jnp.bfloat16)
    values = value_features.astype(jnp.bfloat16).reshape(SEQ, KV_HEADS, HEAD_DIM)
    by_head_queries = jnp.transpose(queries, (1, 0, 2))
    key_heads = jnp.transpose(keys, (1, 0, 2))
    value_heads = jnp.transpose(values, (1, 0, 2))
    group_size = HEADS // KV_HEADS
    allowed = positions[None, :] <= positions[:, None]
    score_scale = 1.0 / math.sqrt(HEAD_DIM)

    def one_head(head_index):
        query_block = lax.dynamic_index_in_dim(by_head_queries, head_index, 0, keepdims=False)
        key_block = lax.dynamic_index_in_dim(key_heads, head_index // group_size, 0, keepdims=False)
        value_block = lax.dynamic_index_in_dim(value_heads, head_index // group_size, 0, keepdims=False)
        scores = jnp.dot(query_block, key_block.T, preferred_element_type=jnp.float32) * score_scale
        scores = jnp.where(allowed, scores, -jnp.inf)
        row_top = lax.optimization_barrier(jnp.max(scores, axis=-1, keepdims=True))
        normalizer = row_top + jnp.log(lax.optimization_barrier(jnp.sum(jnp.exp(scores - row_top), axis=-1, keepdims=True)))
        weights = jnp.exp(scores - normalizer).astype(jnp.bfloat16)
        attended_head = jnp.dot(weights, value_block, preferred_element_type=jnp.float32).astype(jnp.bfloat16)
        return (attended_head, normalizer[:, 0])
    attended, log_normalizer = lax.map(one_head, jnp.arange(HEADS, dtype=jnp.int32))
    attended_flat = jnp.transpose(attended, (1, 0, 2)).reshape(SEQ, HEADS * HEAD_DIM)
    group_rows = HEADS * HEAD_DIM // N_TP
    attended_groups = jnp.transpose(attended_flat.reshape(SEQ, N_TP, group_rows), (1, 0, 2))
    weight_groups = output_weight.reshape(N_TP, group_rows, D)

    def add_group(running_total, pieces):
        group_term = jnp.dot(pieces[0], pieces[1], preferred_element_type=jnp.float32).astype(jnp.bfloat16)
        group_term = lax.optimization_barrier(group_term)
        return (running_total + group_term.astype(jnp.float32), None)
    running_total, unused = lax.scan(add_group, jnp.zeros((SEQ, D), jnp.float32), (attended_groups, weight_groups))
    return (running_total.astype(jnp.bfloat16), log_normalizer)
```

```python
import functools
import math

import jax
import jax.numpy as jnp
from jax import lax
from jax.experimental import pallas as pl
from jax.experimental.pallas import tpu as pltpu
from jax.sharding import PartitionSpec as P


KV_HEADS = 8
HEAD_DIM = 128


rope_base = 500000.0
norm_epsilon = 1e-05
masked_score = -1e30
f32 = jnp.float32
bf16 = jnp.bfloat16
VMEM = 50 * 2**20


def flip(block, axis, mask):
    count = lax.axis_size(axis)
    return lax.ppermute(block, axis, [(i, i ^ mask) for i in range(count)])


def from_behind(block, axis, distance):
    devices = range(lax.axis_size(axis))
    route = [((i - distance) % len(devices), i) for i in devices]
    return lax.ppermute(block, axis, route)


def rope_tables(positions):
    lane = jnp.arange(HEAD_DIM, dtype=jnp.int32)
    pair_index = (lane // 2).astype(f32)
    inverse_rates = rope_base ** (-2.0 * pair_index / HEAD_DIM)
    angles = positions.astype(f32)[:, None] * inverse_rates[None, :]
    sine = jnp.sin(angles)
    return jnp.cos(angles), jnp.where(lane % 2 == 0, -sine, sine)


def normalise(rank, gains, first, pieces, weights, carry=None, tables=None):
    count = len(pieces)
    rows = sum(r for _, _, r in pieces[0])
    width = pieces[0][0][0].shape[1]
    flat = [part for piece in pieces for part, _, _ in piece]
    most = max(len(piece) for piece in pieces)
    total_width = gains.shape[0] * width
    columns = sum(w.shape[1] for w, _ in weights)
    n = len(weights)
    given = list(carry or []) + list(tables or [])
    ahead = min(count, 3)

    def body(rank_ref, gain_ref, *refs):
        piece_refs, refs = refs[: len(flat)], refs[len(flat) :]
        weight_refs, refs = refs[:n], refs[n:]
        given_refs, refs = refs[: len(given)], refs[len(given) :]
        scaled, product, *others = refs[: 4 if tables else 3]
        taken, held, total, squares, taken_sems, held_sems = refs[4 if tables else 3 :]

        def fetch(j):
            at = sum(len(piece) for piece in pieces[:j])
            row = 0
            for p, (_, start, size) in enumerate(pieces[j]):
                source = piece_refs[at + p].at[pl.ds(start, size)]
                yield pltpu.make_async_copy(source, taken.at[j, pl.ds(row, size)], taken_sems.at[j, p])
                row += size
            start = pl.multiple_of((rank_ref[0] ^ (first + j)) * width, width)
            column = 0
            for i, (w, _) in enumerate(weights):
                size = w.shape[1]
                target = held.at[j, :, pl.ds(column, size)]
                yield pltpu.make_async_copy(weight_refs[i].at[pl.ds(start, width)], target, held_sems.at[i, j])
                column += size

        def begin(j):
            for copy in fetch(j):
                copy.start()

        for j in range(ahead):
            begin(j)
        if carry:
            total[...] = given_refs[0][...]
            squares[...] = given_refs[1][...]
        else:
            total[...] = jnp.zeros_like(total)
            squares[...] = jnp.zeros_like(squares)

        def step(j, _):
            for m in range(count):

                @pl.when(j == m)
                def _(m=m):
                    if m + ahead < count:
                        begin(m + ahead)
                    for copy in fetch(m):
                        copy.wait()

            gain = gain_ref[rank_ref[0] ^ (first + j)]
            for r in range(0, rows, 32):
                x = taken[j, r : r + 32].astype(f32)
                scaled[j, r : r + 32] = (x * gain).astype(bf16)
                square = x * x
                part = square[:, :128]
                for c in range(128, width, 128):
                    part = part + square[:, c : c + 128]
                squares[r : r + 32] += part
            total[...] += jnp.dot(scaled[j], held[j], preferred_element_type=f32)
            return 0

        lax.fori_loop(0, count, step, 0)
        if not tables:
            product[...] = total[...]
            others[0][...] = squares[...]
            return
        mean = jnp.sum(squares[...], axis=1, keepdims=True) / total_width
        r = lax.rsqrt(mean + norm_epsilon)
        cos_ref, sin_ref = given_refs[-2:]
        cr, sr = cos_ref[...] * r, sin_ref[...] * r
        others[0][...] = cr
        others[1][...] = sr
        column = 0
        for w, rotated in weights:
            for c in range(column, column + w.shape[1], HEAD_DIM):
                a = total[:, c : c + HEAD_DIM]
                a = turn(a, cr, sr) if rotated else a * r
                product[:, c : c + HEAD_DIM] = a.astype(bf16)
            column += w.shape[1]

    whole = lambda shape: pl.BlockSpec(shape, lambda i, t: (0,) * len(shape))
    far = pl.BlockSpec(memory_space=pltpu.MemorySpace.HBM)
    out_shape = [jax.ShapeDtypeStruct((count, rows, width), bf16)]
    if tables:
        out_shape += [jax.ShapeDtypeStruct((rows, columns), bf16)] + [jax.ShapeDtypeStruct((rows, HEAD_DIM), f32)] * 2
    else:
        out_shape += [jax.ShapeDtypeStruct((rows, c), f32) for c in (columns, 128)]
    grid_spec = pltpu.PrefetchScalarGridSpec(
        num_scalar_prefetch=1,
        grid=(1,),
        in_specs=[whole(gains.shape)] + [far] * (len(flat) + n) + [whole(g.shape) for g in given],
        out_specs=[whole(o.shape) for o in out_shape],
        scratch_shapes=[
            pltpu.VMEM((count, rows, width), bf16),
            pltpu.VMEM((count, width, columns), bf16),
            pltpu.VMEM((rows, columns), f32),
            pltpu.VMEM((rows, 128), f32),
            pltpu.SemaphoreType.DMA((count, most)),
            pltpu.SemaphoreType.DMA((n, count)),
        ],
    )
    return pl.pallas_call(
        body,
        grid_spec=grid_spec,
        out_shape=out_shape,
        compiler_params=pltpu.CompilerParams(vmem_limit_bytes=VMEM),
        cost_estimate=pl.CostEstimate(
            flops=2 * rows * count * width * columns,
            bytes_accessed=2 * count * width * (rows + columns),
            transcendentals=0,
        ),
        name="normalise",
    )(rank, gains, *flat, *[w for w, _ in weights], *given)


def turn(a, cosine, sine):
    even = lax.broadcasted_iota(jnp.int32, a.shape, 1) % 2 == 0
    other = jnp.where(even, pltpu.roll(a, HEAD_DIM - 1, 1), pltpu.roll(a, 1, 1))
    return a * cosine + other * sine


def project(rank, chunks, weight):
    rows, width = chunks[0][0][0].shape[1:]
    sizes = [s.shape[0] for s in chunks[0][0]]
    count = sum(sizes)
    columns = weight.shape[1]
    ahead = 4
    n = len(chunks)

    def body(rank_ref, *refs):
        table_refs, refs = refs[: 2 * n], refs[2 * n :]
        scaled_refs, refs = refs[: n * len(sizes)], refs[n * len(sizes) :]
        weight_ref, *outs = refs[: 1 + n]
        held, total, sems = refs[1 + n :]

        def fetch(j):
            start = pl.multiple_of((rank_ref[0] ^ j) * width, width)
            slot = j % ahead
            return pltpu.make_async_copy(weight_ref.at[pl.ds(start, width)], held.at[slot], sems.at[slot])

        for j in range(ahead - 1):
            fetch(j).start()
        total[...] = jnp.zeros_like(total)
        first = 0
        for i, size in enumerate(sizes):

            def step(j, _, i=i, first=first):
                @pl.when(j + ahead - 1 < count)
                def _():
                    fetch(j + ahead - 1).start()

                fetch(j).wait()
                for c in range(n):
                    lhs = scaled_refs[c * len(sizes) + i][j - first]
                    total[c] += jnp.dot(lhs, held[j % ahead], preferred_element_type=f32)
                return 0

            lax.fori_loop(first, first + size, step, 0)
            first += size
        for i in range(n):
            for c in range(0, columns, HEAD_DIM):
                a = turn(total[i, :, c : c + HEAD_DIM], table_refs[2 * i][...], table_refs[2 * i + 1][...])
                outs[i][:, c : c + HEAD_DIM] = a.astype(bf16)

    tables = [t for _, *pair in chunks for t in pair]
    scaled = [s for pieces, _, _ in chunks for s in pieces]
    whole = lambda shape: pl.BlockSpec(shape, lambda i, t: (0,) * len(shape))
    grid_spec = pltpu.PrefetchScalarGridSpec(
        num_scalar_prefetch=1,
        grid=(1,),
        in_specs=[whole(t.shape) for t in tables]
        + [whole(s.shape) for s in scaled]
        + [pl.BlockSpec(memory_space=pltpu.MemorySpace.HBM)],
        out_specs=[whole((rows, columns))] * n,
        scratch_shapes=[
            pltpu.VMEM((ahead, width, columns), bf16),
            pltpu.VMEM((n, rows, columns), f32),
            pltpu.SemaphoreType.DMA((ahead,)),
        ],
    )
    return pl.pallas_call(
        body,
        grid_spec=grid_spec,
        out_shape=[jax.ShapeDtypeStruct((rows, columns), bf16)] * n,
        compiler_params=pltpu.CompilerParams(vmem_limit_bytes=VMEM),
        cost_estimate=pl.CostEstimate(
            flops=2 * n * rows * count * width * columns, bytes_accessed=2 * count * width * columns, transcendentals=0
        ),
        name="project",
    )(rank, *tables, *scaled, weight)


def attend(queries, slot, block_order, context_rank, pieces):
    rows = queries.shape[0]
    heads = queries.shape[1] // HEAD_DIM
    key_rows = pieces[0].shape[0]
    tile = min(rows, key_rows, 256)
    q_tiles, k_tiles = rows // tile, key_rows // tile
    factor = math.log2(math.e) / math.sqrt(HEAD_DIM)
    n = len(pieces)
    sources = n // 2

    def body(order_ref, place_ref, q_ref, *refs):
        piece_refs = refs[:n]
        outs = refs[n:-5]
        keys, values, top, total, acc = refs[-5:]
        step = pl.program_id(0)

        @pl.when(step == 0)
        def _():
            top[...] = jnp.full_like(top, masked_score)
            total[...] = jnp.zeros_like(total)
            acc[...] = jnp.zeros_like(acc)

        for j in range(n):

            @pl.when(step == j)
            def _(j=j):
                keys[...] = piece_refs[j][:, :HEAD_DIM]
                values[...] = piece_refs[j][:, HEAD_DIM:].T

        ahead = lax.broadcasted_iota(jnp.int32, (tile, tile), 0) - lax.broadcasted_iota(jnp.int32, (tile, tile), 1)
        for ki in range(k_tiles):
            source = (place_ref[0] - step // 2 + sources) % sources
            k0 = order_ref[2 * source + step % 2] * key_rows + ki * tile
            for qi in range(q_tiles):
                q0 = order_ref[2 * place_ref[0] + slot] * rows + qi * tile
                span = slice(qi * tile, (qi + 1) * tile)

                @pl.when(k0 <= q0 + tile - 1)
                def _(ki=ki, k0=k0, q0=q0, span=span):
                    k = keys[ki * tile : (ki + 1) * tile]
                    v = values[:, ki * tile : (ki + 1) * tile]

                    held = []
                    for h in range(heads):
                        q = q_ref[span, h * HEAD_DIM : (h + 1) * HEAD_DIM]
                        s = lax.dot_general(k, q, (((1,), (1,)), ((), ())), preferred_element_type=f32)
                        held.append(jnp.where(ahead <= q0 - k0, s * factor, masked_score))
                    for h in range(heads):
                        old = top[h, :, span]
                        new = jnp.maximum(old, jnp.max(held[h], axis=0, keepdims=True))
                        p = jnp.exp2(held[h] - new)
                        shrink = jnp.exp2(old - new)
                        top[h, :, span] = new
                        total[h, :, span] = total[h, :, span] * shrink + jnp.sum(p, axis=0, keepdims=True)
                        held[h] = (p.astype(bf16), shrink)
                    for h in range(heads):
                        p, shrink = held[h]
                        acc[h, :, span] = acc[h, :, span] * shrink + jnp.dot(v, p, preferred_element_type=f32)

        @pl.when(step == n - 1)
        def _():
            for h in range(heads):
                t = total[h]
                outs[1][h] = (top[h] + jnp.log2(t)) * math.log(2.0)
                outs[0][:, h * HEAD_DIM : (h + 1) * HEAD_DIM] = (acc[h] / t).T.astype(bf16)

    small = (heads, 1, rows)
    big = (heads, HEAD_DIM, rows)
    whole = lambda shape: pl.BlockSpec(shape, lambda i, a, b: (0,) * len(shape))
    out_shape = [jax.ShapeDtypeStruct(queries.shape, bf16), jax.ShapeDtypeStruct(small, f32)]
    grid_spec = pltpu.PrefetchScalarGridSpec(
        num_scalar_prefetch=2,
        grid=(n,),
        in_specs=[whole(queries.shape)] + [whole(p.shape) for p in pieces],
        out_specs=[whole(o.shape) for o in out_shape],
        scratch_shapes=[
            pltpu.VMEM((key_rows, HEAD_DIM), bf16),
            pltpu.VMEM((HEAD_DIM, key_rows), bf16),
            pltpu.VMEM(small, f32),
            pltpu.VMEM(small, f32),
            pltpu.VMEM(big, f32),
        ],
    )
    return pl.pallas_call(
        body,
        grid_spec=grid_spec,
        out_shape=out_shape,
        compiler_params=pltpu.CompilerParams(vmem_limit_bytes=VMEM),
        cost_estimate=pl.CostEstimate(
            flops=4 * rows * heads * n * key_rows * HEAD_DIM,
            bytes_accessed=2 * rows * heads * HEAD_DIM,
            transcendentals=rows * heads * n * key_rows,
        ),
        name="attend",
    )(block_order, context_rank, queries, *pieces)


def spread(rank, slots, own, other, own_weight, other_weight):
    rows, inner = own.shape
    half = rows // 2
    width = other_weight[0].shape[1]
    n = len(slots)
    cuts = 2
    deep = inner // cuts

    def body(rank_ref, a_ref, b_ref, w_ref, *refs):
        other_refs, refs = refs[:n], refs[n:]
        outs, (held, sems) = refs[: 2 * n], refs[2 * n :]

        def hold(j, side, c):
            start = pl.multiple_of((rank_ref[0] ^ (2 * slots[j])) * width, width)
            depth = pl.ds(c * deep, deep)
            source = other_refs[j].at[depth] if side else w_ref.at[depth, pl.ds(start, width)]
            return pltpu.make_async_copy(source, held.at[j, side, depth], sems.at[j, side, c])

        order = [(j, side, c) for j in range(n) for side in range(2) for c in range(cuts)]
        ahead = 3
        for key in order[:ahead]:
            hold(*key).start()
        for j in range(n):
            full = None
            for side, ref in enumerate((a_ref, b_ref)):
                for c in range(cuts):
                    at = order.index((j, side, c)) + ahead
                    if at < len(order):
                        hold(*order[at]).start()
                    hold(j, side, c).wait()
                    cut = slice(c * deep, (c + 1) * deep)
                    term = jnp.dot(ref[:, cut], held[j, side, cut], preferred_element_type=f32)
                    full = term if full is None else full + term
            outs[2 * j][...] = full[:half].astype(bf16)
            outs[2 * j + 1][...] = full[half:].astype(bf16)

    whole = lambda shape: pl.BlockSpec(shape, lambda i, t: (0,) * len(shape))
    far = pl.BlockSpec(memory_space=pltpu.MemorySpace.HBM)
    grid_spec = pltpu.PrefetchScalarGridSpec(
        num_scalar_prefetch=1,
        grid=(1,),
        in_specs=[whole(own.shape), whole(other.shape)] + [far] * (1 + n),
        out_specs=[whole((half, width))] * (2 * n),
        scratch_shapes=[pltpu.VMEM((n, 2, inner, width), bf16), pltpu.SemaphoreType.DMA((n, 2, cuts))],
    )
    return pl.pallas_call(
        body,
        grid_spec=grid_spec,
        out_shape=[jax.ShapeDtypeStruct((half, width), bf16)] * (2 * n),
        compiler_params=pltpu.CompilerParams(vmem_limit_bytes=VMEM),
        cost_estimate=pl.CostEstimate(
            flops=4 * rows * inner * width * n, bytes_accessed=4 * inner * width * n, transcendentals=0
        ),
        name="spread",
    )(rank, own, other, own_weight, *other_weight)


def after(value, *others):
    return lax.optimization_barrier((value, *others))[0]


def plane_shards(checkpoint, norm_gain, query_weight, key_weight, value_weight, output_weight, block_order):
    tok_rows, width = checkpoint.shape
    block_rows = tok_rows // 2
    context_rank = lax.axis_index("cp")
    context_size = lax.axis_size("cp")
    tensor_rank = lax.axis_index("tp")
    rank = tensor_rank.astype(jnp.int32)[None]
    row_offsets = jnp.arange(block_rows, dtype=jnp.int32)
    own_blocks = lax.dynamic_slice_in_dim(block_order, 2 * context_rank, 2)
    positions = (own_blocks[:, None] * block_rows + row_offsets[None, :]).reshape(tok_rows)
    gains = norm_gain.reshape(-1, 1, width)
    CORE, X, Y = 1, 2, 4

    def tp(block, mask):
        return flip(block, "tp", mask)

    half = block_rows // 2
    own_core = tp(checkpoint, CORE)

    gathered = []
    for n in range(2):
        start = n * block_rows
        if n:
            checkpoint_later = after(checkpoint, gathered[0][4][0][0])
        else:
            checkpoint_later = checkpoint
        lo = checkpoint_later[start : start + half]
        hi = checkpoint_later[start + half : start + block_rows]
        x_hi, y_lo = tp(hi, X), tp(lo, Y)
        x_lo, y_hi = tp(lo, X), tp(hi, Y)
        d_lo, d_hi = tp(y_lo, X), tp(x_hi, Y)
        pieces = [[(checkpoint, start, block_rows)], [(own_core, start, block_rows)]]
        for part in ((x_lo, x_hi), (y_lo, y_hi), (d_lo, d_hi)):
            pieces.append([(p, 0, half) for p in part])
            pieces.append([(tp(p, CORE), 0, half) for p in part])
        gathered.append(pieces)

    later = output_weight
    other_weight = []
    for slot in range(lax.axis_size("tp") // 2):
        column = ((tensor_rank ^ CORE) ^ (2 * slot)) * width
        other_weight.append(lax.dynamic_slice_in_dim(later, column, width, 1))
    other_weight = [tp(w, CORE) for w in other_weight]

    cosine, sine = rope_tables(positions)
    tables = [(cosine[n * block_rows : (n + 1) * block_rows], sine[n * block_rows : (n + 1) * block_rows]) for n in range(2)]
    key_value = [(key_weight, True), (value_weight, False)]
    early = 6

    chunks, context = [], []
    for n in range(2):
        scaled, *sums = normalise(rank, gains, 0, gathered[n][:early], key_value)
        rest, own, cosine, sine = normalise(rank, gains, early, gathered[n][early:], key_value, sums, tables[n])
        others = []
        for d in range(1, context_size):
            others.append(from_behind(own, "cp", d))
        context.append([own, *others])
        chunks.append(([scaled, rest], cosine, sine))
    queries = project(rank, chunks, query_weight)

    place = context_rank.astype(jnp.int32)[None]
    pieces = [piece for pair in zip(*context) for piece in pair]
    results, normalizers = [], []
    for c in range(2):
        attended, normalizer = attend(queries[c], c, block_order, place, pieces)
        normalizers.append(normalizer[:, 0])
        partner = tp(attended, CORE)

        def deliver(slots):
            return spread(rank, slots, attended, partner, output_weight, [other_weight[s] for s in slots])

        d_lo, d_hi = deliver([3])
        d_lo, d_hi = tp(d_lo, X), tp(d_hi, Y)
        x_lo, x_hi, y_lo, y_hi = deliver([1, 2])
        s_lo, s_hi = deliver([0])
        add = lambda *terms: functools.reduce(jnp.add, [t.astype(f32) for t in terms])
        x_lo, y_hi = tp(x_lo, X), tp(y_hi, Y)
        x_hi = tp(add(x_hi, d_hi).astype(bf16), X)
        y_lo = tp(add(y_lo, d_lo).astype(bf16), Y)
        results.append(add(s_lo, x_lo, y_lo).astype(bf16))
        results.append(add(s_hi, x_hi, y_hi).astype(bf16))
    return jnp.concatenate(results, axis=0), jnp.concatenate(normalizers, axis=1)


def partner_2(block, axis, stride):
    count = lax.axis_size(axis)
    route = []
    for low in range(count):
        high = low | 1 << stride
        if high != low and high < count:
            route += [(low, high), (high, low)]
    return lax.ppermute(block, axis, route)


def turn_pairs(matrix, positions, first_pair):
    pair_count = matrix.shape[-1] // 2
    pair_index = (first_pair + jnp.arange(pair_count, dtype=jnp.int32)).astype(jnp.float32)
    inverse_rates = rope_base ** (-2.0 * pair_index / HEAD_DIM)
    angles = positions.astype(jnp.float32)[:, None] * inverse_rates[None, :]
    cosine = jnp.cos(angles)[:, None, :]
    sine_part = jnp.sin(angles)[:, None, :]
    paired = matrix.reshape(matrix.shape[0], matrix.shape[1], pair_count, 2)
    former = paired[..., 0]
    latter = paired[..., 1]
    turned = jnp.stack(
        [former * cosine - latter * sine_part, former * sine_part + latter * cosine], axis=-1
    )
    return turned.reshape(matrix.shape)


def shards(
    checkpoint, norm_gain, query_weight, key_weight, value_weight, output_weight, block_order
):
    tok_rows = checkpoint.shape[0]
    block_rows = tok_rows // 2
    local_heads = query_weight.shape[1] // HEAD_DIM
    key_columns = key_weight.shape[1]
    context_rank = lax.axis_index("cp")
    tensor_rank = lax.axis_index("tp")
    row_offsets = jnp.arange(block_rows, dtype=jnp.int32)
    own_blocks = lax.dynamic_slice_in_dim(block_order, 2 * context_rank, 2)
    own_positions = (own_blocks[:, None] * block_rows + row_offsets[None, :]).reshape(tok_rows)
    gathered = lax.all_gather(checkpoint, "tp", axis=1, tiled=True)
    widened = gathered.astype(jnp.float32)
    mean_square = jnp.mean(widened * widened, axis=-1, keepdims=True)
    normed = (widened * lax.rsqrt(mean_square + norm_epsilon) * norm_gain).astype(jnp.bfloat16)
    query_features = jnp.dot(normed, query_weight, preferred_element_type=jnp.float32)
    key_features = jnp.dot(normed, key_weight, preferred_element_type=jnp.float32)
    value_features = jnp.dot(normed, value_weight, preferred_element_type=jnp.float32)
    queries = turn_pairs(
        query_features.reshape(tok_rows, local_heads, HEAD_DIM), own_positions, 0
    ).astype(jnp.bfloat16)
    sharing = lax.axis_size("tp") // KV_HEADS
    part_of_head = tensor_rank % sharing
    key_part = turn_pairs(
        key_features.reshape(tok_rows, 1, key_columns),
        own_positions,
        part_of_head * (key_columns // 2),
    )
    key_part = key_part.astype(jnp.bfloat16).reshape(tok_rows, key_columns)
    value_part = value_features.astype(jnp.bfloat16)
    own_pair = jnp.stack([key_part, value_part])
    if sharing == 2:
        partner = partner_2(own_pair, "tp", 0)
        lower_first = jnp.concatenate([own_pair, partner], axis=-1)
        upper_first = jnp.concatenate([partner, own_pair], axis=-1)
        key_value = jnp.where(part_of_head == 0, lower_first, upper_first)
    else:
        key_value = own_pair
    score_scale = 1.0 / math.sqrt(HEAD_DIM)

    def absorb(running, query_slot, key_block, key_rows, value_rows):
        query_block = own_blocks[query_slot]
        top_scores, totals, weighted = running
        query_rows = queries[query_slot * block_rows : (query_slot + 1) * block_rows]
        scores = (
            jnp.einsum("qhd,kd->qhk", query_rows, key_rows, preferred_element_type=jnp.float32)
            * score_scale
        )
        query_places = query_block * block_rows + row_offsets
        key_places = key_block * block_rows + row_offsets
        allowed = (key_places[None, :] <= query_places[:, None])[:, None, :]
        scores = jnp.where(allowed, scores, masked_score)
        old_top = top_scores[query_slot]
        new_top = jnp.maximum(old_top, jnp.max(scores, axis=-1))
        weights = jnp.where(allowed, jnp.exp(scores - new_top[..., None]), 0.0)
        shrink = jnp.exp(old_top - new_top)
        new_total = totals[query_slot] * shrink + jnp.sum(weights, axis=-1)
        new_sum = weighted[query_slot] * shrink[..., None] + jnp.einsum(
            "qhk,kd->qhd",
            weights.astype(jnp.bfloat16),
            value_rows,
            preferred_element_type=jnp.float32,
        )
        return (
            top_scores.at[query_slot].set(new_top),
            totals.at[query_slot].set(new_total),
            weighted.at[query_slot].set(new_sum),
        )

    def visit_rows(running, key_value_rows, first_row):
        block_count = key_value_rows.shape[1] // block_rows

        def one_block(block_index, current):
            rows_here = lax.dynamic_slice_in_dim(
                key_value_rows, block_index * block_rows, block_rows, 1
            )
            stored = first_row // block_rows + block_index
            key_block = lax.dynamic_index_in_dim(block_order, stored, 0, keepdims=False)
            for query_slot in range(2):
                current = absorb(current, query_slot, key_block, rows_here[0], rows_here[1])
            return current

        return lax.fori_loop(0, block_count, one_block, running)

    running = (
        jnp.full((2, block_rows, local_heads), masked_score, jnp.float32),
        jnp.zeros((2, block_rows, local_heads), jnp.float32),
        jnp.zeros((2, block_rows, local_heads, HEAD_DIM), jnp.float32),
    )
    running = visit_rows(running, key_value, context_rank * tok_rows)
    context_size = lax.axis_size("cp")

    def pass_turn(turn_index, carried):
        current, travelling = carried
        travelling = from_behind(travelling, "cp", 1)
        source = (context_rank - turn_index) % context_size
        return (visit_rows(current, travelling, source * tok_rows), travelling)

    running, _ = lax.fori_loop(1, context_size, pass_turn, (running, key_value))
    top_scores, totals, weighted = running
    attended = (
        (weighted / totals[..., None])
        .astype(jnp.bfloat16)
        .reshape(tok_rows, local_heads * HEAD_DIM)
    )
    normalizer = jnp.transpose((top_scores + jnp.log(totals)).reshape(tok_rows, local_heads))
    partial_terms = jnp.dot(attended, output_weight, preferred_element_type=jnp.float32)
    projected = lax.psum_scatter(
        partial_terms.astype(jnp.bfloat16), "tp", scatter_dimension=1, tiled=True
    )
    return (projected, normalizer)


def solution(mesh):
    plane = mesh.shape["tp"] == KV_HEADS

    def body(*args):
        return plane_shards(*args)

    return jax.shard_map(
        body if plane else shards,
        mesh=mesh,
        in_specs=(
            P("cp", "tp"),
            P(),
            P(None, "tp"),
            P(None, "tp"),
            P(None, "tp"),
            P("tp", None),
            P(),
        ),
        out_specs=(P("cp", "tp"), P("tp", "cp")),
        check_vma=False,
    )
```

```python
import functools
import math

import jax
import jax.numpy as jnp
from jax import lax
from jax.experimental import pallas as pl
from jax.experimental.pallas import tpu as pltpu
from jax.sharding import PartitionSpec as P


KV_HEADS = 8
HEAD_DIM = 128


rope_base = 500000.0
norm_epsilon = 1e-05
masked_score = -1e30
score_factor = math.log2(math.e) / math.sqrt(HEAD_DIM)
f32 = jnp.float32
bf16 = jnp.bfloat16


def flip(block, axis, mask):
    count = lax.axis_size(axis)
    return lax.ppermute(block, axis, [(i, i ^ mask) for i in range(count)])


def from_behind(block, axis, distance):
    devices = range(lax.axis_size(axis))
    route = [((i - distance) % len(devices), i) for i in devices]
    return lax.ppermute(block, axis, route)


def rope_tables(positions):
    lane = jnp.arange(HEAD_DIM, dtype=jnp.int32)
    pair_index = (lane // 2).astype(f32)
    inverse_rates = rope_base ** (-2.0 * pair_index / HEAD_DIM)
    angles = positions.astype(f32)[:, None] * inverse_rates[None, :]
    sine = jnp.sin(angles)
    return jnp.cos(angles), jnp.where(lane % 2 == 0, -sine, sine)


def begin(rank, gains, first, pieces, weights, chunks, carry=()):
    count = len(pieces)
    rows, width = pieces[0].shape
    part = rows // chunks
    wide = weights[0].shape[1]
    narrow = [w.shape[1] for w in weights[1:]]

    def body(rank_ref, gain_ref, *refs):
        piece_refs, refs = refs[:count], refs[count:]
        weight_refs, refs = refs[:3], refs[3:]
        carry_refs, refs = refs[: len(carry)], refs[len(carry) :]
        outs, refs = refs[: 3 * chunks], refs[3 * chunks :]
        taken, scaled, held, held_pair, total, pair, squares, sems = refs

        def fetch(j):
            start = pl.multiple_of((rank_ref[0] ^ (first + j)) * width, width)
            yield pltpu.make_async_copy(piece_refs[j], taken.at[j], sems.at[j, 0])
            yield pltpu.make_async_copy(weight_refs[0].at[pl.ds(start, width)], held.at[j], sems.at[j, 1])
            column = 0
            for i, size in enumerate(narrow):
                target = held_pair.at[j, :, pl.ds(column, size)]
                yield pltpu.make_async_copy(weight_refs[1 + i].at[pl.ds(start, width)], target, sems.at[j, 2 + i])
                column += size

        for j in range(count):
            for copy in fetch(j):
                copy.start()
        for i, ref in enumerate((total, pair, squares)):
            for c in range(chunks):
                here = slice(c * part, (c + 1) * part)
                ref[here] = carry_refs[3 * c + i][...] if carry else jnp.zeros((part, ref.shape[1]), f32)

        def step(j, _):
            for m in range(count):

                @pl.when(j == m)
                def _(m=m):
                    for copy in fetch(m):
                        copy.wait()

            gain = gain_ref[rank_ref[0] ^ (first + j)]

            def some(c, _):
                for r in range(0, 128, 32):
                    here = pl.ds(pl.multiple_of(c * 128 + r, 32), 32)
                    x = taken[j, here].astype(f32)
                    scaled[here] = (x * gain).astype(bf16)
                    square = x * x
                    sums = square[:, :128]
                    for k in range(128, width, 128):
                        sums = sums + square[:, k : k + 128]
                    squares[here] += sums
                return 0

            lax.fori_loop(0, rows // 128, some, 0)
            for c in range(chunks):
                here = slice(c * part, (c + 1) * part)
                total[here] += jnp.dot(scaled[here], held[j], preferred_element_type=f32)
                pair[here] += jnp.dot(scaled[here], held_pair[j], preferred_element_type=f32)
            return 0

        lax.fori_loop(0, count, step, 0)
        for c in range(chunks):
            for i, ref in enumerate((total, pair, squares)):
                outs[3 * c + i][...] = ref[c * part : (c + 1) * part]

    far = pl.BlockSpec(memory_space=pltpu.MemorySpace.HBM)
    whole = lambda shape: pl.BlockSpec(shape, lambda i, t: (0,) * len(shape))
    widths = [wide, sum(narrow), 128]
    grid_spec = pltpu.PrefetchScalarGridSpec(
        num_scalar_prefetch=1,
        grid=(1,),
        in_specs=[whole(gains.shape)] + [far] * (count + 3) + [whole(c.shape) for c in carry],
        out_specs=[whole((part, c)) for _ in range(chunks) for c in widths],
        scratch_shapes=[
            pltpu.VMEM((count, rows, width), bf16),
            pltpu.VMEM((rows, width), bf16),
            pltpu.VMEM((count, width, wide), bf16),
            pltpu.VMEM((count, width, sum(narrow)), bf16),
        ]
        + [pltpu.VMEM((rows, c), f32) for c in widths]
        + [pltpu.SemaphoreType.DMA((count, 4))],
    )
    return pl.pallas_call(
        body,
        grid_spec=grid_spec,
        out_shape=[jax.ShapeDtypeStruct((part, c), f32) for _ in range(chunks) for c in widths],
        compiler_params=pltpu.CompilerParams(vmem_limit_bytes=46 * 2**20),
        cost_estimate=pl.CostEstimate(
            flops=2 * rows * count * width * (wide + sum(narrow)),
            bytes_accessed=2 * count * width * (rows + wide + sum(narrow)),
            transcendentals=0,
        ),
        name="begin",
    )(rank, gains, *pieces, *weights, *carry)


def normalise(rank, gains, first, pieces, weights, carry=None, tables=None, start_row=0):
    count = len(pieces)
    rows = sum(r for _, _, r in pieces[0])
    width = pieces[0][0][0].shape[1]
    flat = [part for piece in pieces for part, _, _ in piece]
    most = max(len(piece) for piece in pieces)
    total_width = gains.shape[0] * width
    columns = sum(w.shape[1] for w, _ in weights)
    n = len(weights)
    given = list(carry or []) + list(tables or [])
    ahead = min(count, 3)

    def body(rank_ref, gain_ref, *refs):
        piece_refs, refs = refs[: len(flat)], refs[len(flat) :]
        weight_refs, refs = refs[:n], refs[n:]
        given_refs, refs = refs[: len(given)], refs[len(given) :]
        scaled, product, *others = refs[: 4 if tables else 3]
        taken, held, total, squares, taken_sems, held_sems = refs[4 if tables else 3 :]

        def fetch(j):
            at = sum(len(piece) for piece in pieces[:j])
            row = 0
            for p, (_, start, size) in enumerate(pieces[j]):
                source = piece_refs[at + p].at[pl.ds(start, size)]
                yield pltpu.make_async_copy(source, taken.at[j, pl.ds(row, size)], taken_sems.at[j, p])
                row += size
            start = pl.multiple_of((rank_ref[0] ^ (first + j)) * width, width)
            column = 0
            for i, (w, _) in enumerate(weights):
                size = w.shape[1]
                target = held.at[j, :, pl.ds(column, size)]
                yield pltpu.make_async_copy(weight_refs[i].at[pl.ds(start, width)], target, held_sems.at[i, j])
                column += size

        def begin(j):
            for copy in fetch(j):
                copy.start()

        for j in range(ahead):
            begin(j)
        if carry:
            total[...] = given_refs[0][...]
            squares[...] = given_refs[1][...]
        else:
            total[...] = jnp.zeros_like(total)
            squares[...] = jnp.zeros_like(squares)

        def step(j, _):
            for m in range(count):

                @pl.when(j == m)
                def _(m=m):
                    if m + ahead < count:
                        begin(m + ahead)
                    for copy in fetch(m):
                        copy.wait()

            gain = gain_ref[rank_ref[0] ^ (first + j)]
            for r in range(0, rows, 32):
                x = taken[j, r : r + 32].astype(f32)
                scaled[j, r : r + 32] = (x * gain).astype(bf16)
                square = x * x
                part = square[:, :128]
                for c in range(128, width, 128):
                    part = part + square[:, c : c + 128]
                squares[r : r + 32] += part
            total[...] += jnp.dot(scaled[j], held[j], preferred_element_type=f32)
            return 0

        lax.fori_loop(0, count, step, 0)
        if not tables:
            product[...] = total[...]
            others[0][...] = squares[...]
            return
        mean = jnp.sum(squares[...], axis=1, keepdims=True) / total_width
        r = lax.rsqrt(mean + norm_epsilon)
        cos_ref, sin_ref = given_refs[-2:]
        cr, sr = cos_ref[start_row : start_row + rows] * r, sin_ref[start_row : start_row + rows] * r
        others[0][...] = cr * score_factor
        others[1][...] = sr * score_factor
        column = 0
        for w, rotated in weights:
            for c in range(column, column + w.shape[1], HEAD_DIM):
                a = total[:, c : c + HEAD_DIM]
                a = turn(a, cr, sr) if rotated else a * r
                product[:, c : c + HEAD_DIM] = a.astype(bf16)
            column += w.shape[1]

    whole = lambda shape: pl.BlockSpec(shape, lambda i, t: (0,) * len(shape))
    far = pl.BlockSpec(memory_space=pltpu.MemorySpace.HBM)
    out_shape = [jax.ShapeDtypeStruct((count, rows, width), bf16)]
    if tables:
        out_shape += [jax.ShapeDtypeStruct((rows, columns), bf16)] + [jax.ShapeDtypeStruct((rows, HEAD_DIM), f32)] * 2
    else:
        out_shape += [jax.ShapeDtypeStruct((rows, c), f32) for c in (columns, 128)]
    grid_spec = pltpu.PrefetchScalarGridSpec(
        num_scalar_prefetch=1,
        grid=(1,),
        in_specs=[whole(gains.shape)] + [far] * (len(flat) + n) + [whole(g.shape) for g in given],
        out_specs=[whole(o.shape) for o in out_shape],
        scratch_shapes=[
            pltpu.VMEM((count, rows, width), bf16),
            pltpu.VMEM((count, width, columns), bf16),
            pltpu.VMEM((rows, columns), f32),
            pltpu.VMEM((rows, 128), f32),
            pltpu.SemaphoreType.DMA((count, most)),
            pltpu.SemaphoreType.DMA((n, count)),
        ],
    )
    return pl.pallas_call(
        body,
        grid_spec=grid_spec,
        out_shape=out_shape,
        compiler_params=pltpu.CompilerParams(vmem_limit_bytes=16 * 2**20),
        cost_estimate=pl.CostEstimate(
            flops=2 * rows * count * width * columns,
            bytes_accessed=2 * count * width * (rows + columns),
            transcendentals=0,
        ),
        name="normalise",
    )(rank, gains, *flat, *[w for w, _ in weights], *given)


def turn(a, cosine, sine):
    even = lax.broadcasted_iota(jnp.int32, a.shape, 1) % 2 == 0
    other = jnp.where(even, pltpu.roll(a, HEAD_DIM - 1, 1), pltpu.roll(a, 1, 1))
    return a * cosine + other * sine


def project(rank, chunks, weight, first_piece, other_weight, blocks):
    rows, width = chunks[0][0][0].shape[1:]
    sizes = [s.shape[0] for s in chunks[0][0]]
    count = sum(sizes)
    columns = weight.shape[1]
    ahead = 4
    n = len(chunks)
    tables = [t for _, *three in chunks for t in three]
    scaled = [s for pieces, *_ in chunks for s in pieces]
    tall = other_weight.shape[0]

    def body(rank_ref, *refs):
        table_refs, refs = refs[: 3 * n], refs[3 * n :]
        scaled_refs, refs = refs[: n * len(sizes)], refs[n * len(sizes) :]
        weight_ref, other_ref, *outs = refs[: 2 + n + len(blocks)]
        held, total, moved, sems, block_sems = refs[2 + n + len(blocks) :]
        copies = []
        for i, block in enumerate(blocks):
            start = pl.multiple_of((rank_ref[0] ^ block) * width, width)
            copies.append(
                (
                    pltpu.make_async_copy(other_ref.at[:, pl.ds(start, width)], moved.at[i], block_sems.at[i, 0]),
                    pltpu.make_async_copy(moved.at[i], outs[n + i], block_sems.at[i, 1]),
                )
            )

        def fetch(j):
            start = pl.multiple_of((rank_ref[0] ^ (first_piece + j)) * width, width)
            slot = j % ahead
            return pltpu.make_async_copy(weight_ref.at[pl.ds(start, width)], held.at[slot], sems.at[slot])

        for j in range(ahead - 1):
            fetch(j).start()
        for copy, _ in copies:
            copy.start()
        for c in range(n):
            total[c] = table_refs[3 * c + 2][...]
        first = 0
        for part, size in enumerate(sizes):

            def step(j, _, part=part, first=first):
                @pl.when(j + ahead - 1 < count)
                def _():
                    fetch(j + ahead - 1).start()

                fetch(j).wait()
                for i, (inward, outward) in enumerate(copies):

                    @pl.when(j == count - len(copies) + i)
                    def _(inward=inward, outward=outward):
                        inward.wait()
                        outward.start()

                for c in range(n):
                    lhs = scaled_refs[c * len(sizes) + part][j - first]
                    total[c] += jnp.dot(lhs, held[j % ahead], preferred_element_type=f32)
                return 0

            lax.fori_loop(first, first + size, step, 0)
            first += size
        for i in range(n):
            for c in range(0, columns, HEAD_DIM):
                a = turn(total[i, :, c : c + HEAD_DIM], table_refs[3 * i][...], table_refs[3 * i + 1][...])
                outs[i][:, c : c + HEAD_DIM] = a.astype(bf16)
        for _, copy in copies:
            copy.wait()

    far = pl.BlockSpec(memory_space=pltpu.MemorySpace.HBM)
    whole = lambda shape: pl.BlockSpec(shape, lambda i, t: (0,) * len(shape))
    grid_spec = pltpu.PrefetchScalarGridSpec(
        num_scalar_prefetch=1,
        grid=(1,),
        in_specs=[whole(t.shape) for t in tables]
        + [whole(s.shape) for s in scaled]
        + [far] * 2,
        out_specs=[whole((rows, columns))] * n + [far] * len(blocks),
        scratch_shapes=[
            pltpu.VMEM((ahead, width, columns), bf16),
            pltpu.VMEM((n, rows, columns), f32),
            pltpu.VMEM((len(blocks), tall, width), bf16),
            pltpu.SemaphoreType.DMA((ahead,)),
            pltpu.SemaphoreType.DMA((len(blocks), 2)),
        ],
    )
    return pl.pallas_call(
        body,
        grid_spec=grid_spec,
        out_shape=[jax.ShapeDtypeStruct((rows, columns), bf16)] * n
        + [jax.ShapeDtypeStruct((tall, width), bf16)] * len(blocks),
        compiler_params=pltpu.CompilerParams(vmem_limit_bytes=34 * 2**20),
        cost_estimate=pl.CostEstimate(
            flops=2 * n * rows * count * width * columns, bytes_accessed=2 * count * width * columns, transcendentals=0
        ),
        name="project",
    )(rank, *tables, *scaled, weight, other_weight)


def attend(queries, slot, block_order, context_rank, pieces):
    rows = queries.shape[0]
    heads = queries.shape[1] // HEAD_DIM
    key_rows = pieces[0].shape[0]
    tile = min(rows, key_rows, 256)
    q_tiles, k_tiles = rows // tile, key_rows // tile
    n = len(pieces)

    def body(order_ref, place_ref, q_ref, *refs):
        piece_refs = refs[:n]
        outs = refs[n:-4]
        keys, values, top, acc = refs[-4:]
        step = pl.program_id(0)

        @pl.when(step == 0)
        def _():
            top[...] = jnp.full_like(top, masked_score)
            acc[...] = jnp.zeros_like(acc)
            values[HEAD_DIM:] = jnp.ones((8, key_rows), bf16)

        for j in range(n):

            @pl.when(step == j)
            def _(j=j):
                keys[...] = piece_refs[j][:, :HEAD_DIM]
                values[:HEAD_DIM] = piece_refs[j][:, HEAD_DIM:].T

        ahead = lax.broadcasted_iota(jnp.int32, (tile, tile), 0) - lax.broadcasted_iota(jnp.int32, (tile, tile), 1)
        for ki in range(k_tiles):
            source = place_ref[0] ^ (step // 2)
            k0 = order_ref[2 * source + step % 2] * key_rows + ki * tile
            for qi in range(q_tiles):
                q0 = order_ref[2 * place_ref[0] + slot] * rows + qi * tile
                span = slice(qi * tile, (qi + 1) * tile)

                @pl.when(k0 <= q0 + tile - 1)
                def _(ki=ki, k0=k0, q0=q0, span=span):
                    k = keys[ki * tile : (ki + 1) * tile]
                    v = values[:, ki * tile : (ki + 1) * tile]

                    held = []
                    for h in range(heads):
                        q = q_ref[span, h * HEAD_DIM : (h + 1) * HEAD_DIM]
                        s = lax.dot_general(k, q, (((1,), (1,)), ((), ())), preferred_element_type=f32)
                        held.append(jnp.where(ahead <= q0 - k0, s, masked_score))
                    for h in range(heads):
                        old = top[h, :, span]
                        new = jnp.maximum(old, jnp.max(held[h], axis=0, keepdims=True))
                        p = jnp.exp2(held[h] - new)
                        shrink = jnp.exp2(old - new)
                        top[h, :, span] = new
                        held[h] = (p.astype(bf16), shrink)
                    for h in range(heads):
                        p, shrink = held[h]
                        acc[h, :, span] = acc[h, :, span] * shrink + jnp.dot(v, p, preferred_element_type=f32)

        @pl.when(step == n - 1)
        def _():
            for h in range(heads):
                t = acc[h, HEAD_DIM : HEAD_DIM + 1]
                outs[1][h] = (top[h] + jnp.log2(t)) * math.log(2.0)
                outs[0][:, h * HEAD_DIM : (h + 1) * HEAD_DIM] = (acc[h, :HEAD_DIM] / t).T.astype(bf16)

    small = (heads, 1, rows)
    big = (heads, HEAD_DIM + 8, rows)
    whole = lambda shape: pl.BlockSpec(shape, lambda i, a, b: (0,) * len(shape))
    out_shape = [jax.ShapeDtypeStruct(queries.shape, bf16), jax.ShapeDtypeStruct(small, f32)]
    grid_spec = pltpu.PrefetchScalarGridSpec(
        num_scalar_prefetch=2,
        grid=(n,),
        in_specs=[whole(queries.shape)] + [whole(p.shape) for p in pieces],
        out_specs=[whole(o.shape) for o in out_shape],
        scratch_shapes=[
            pltpu.VMEM((key_rows, HEAD_DIM), bf16),
            pltpu.VMEM((HEAD_DIM + 8, key_rows), bf16),
            pltpu.VMEM(small, f32),
            pltpu.VMEM(big, f32),
        ],
    )
    return pl.pallas_call(
        body,
        grid_spec=grid_spec,
        out_shape=out_shape,
        compiler_params=pltpu.CompilerParams(vmem_limit_bytes=16 * 2**20),
        cost_estimate=pl.CostEstimate(
            flops=4 * rows * heads * n * key_rows * HEAD_DIM,
            bytes_accessed=2 * rows * heads * HEAD_DIM,
            transcendentals=rows * heads * n * key_rows,
        ),
        name="attend",
    )(block_order, context_rank, queries, *pieces)


def spread(rank, slots, own, other, own_weight, other_weight):
    rows, inner = own.shape
    half = rows // 2
    width = other_weight[0].shape[1]
    n = len(slots)
    cuts = 2
    ahead = 4
    deep = inner // cuts

    def body(rank_ref, a_ref, b_ref, w_ref, *refs):
        other_refs, refs = refs[:n], refs[n:]
        outs, (held, sems) = refs[: 2 * n], refs[2 * n :]

        def hold(j, c):
            start = pl.multiple_of((rank_ref[0] ^ (2 * slots[j])) * width, width)
            depth = pl.ds(c * deep, deep)
            return pltpu.make_async_copy(w_ref.at[depth, pl.ds(start, width)], held.at[j, depth], sems.at[j, c])

        order = [(j, c) for j in range(n) for c in range(cuts)]
        for key in order[:ahead]:
            hold(*key).start()
        for j in range(n):
            full = jnp.dot(b_ref[...], other_refs[j][...], preferred_element_type=f32)
            for c in range(cuts):
                at = order.index((j, c)) + ahead
                if at < len(order):
                    hold(*order[at]).start()
                hold(j, c).wait()
                cut = slice(c * deep, (c + 1) * deep)
                full += jnp.dot(a_ref[:, cut], held[j, cut], preferred_element_type=f32)
            outs[2 * j][...] = full[:half].astype(bf16)
            outs[2 * j + 1][...] = full[half:].astype(bf16)

    whole = lambda shape: pl.BlockSpec(shape, lambda i, t: (0,) * len(shape))
    far = pl.BlockSpec(memory_space=pltpu.MemorySpace.HBM)
    grid_spec = pltpu.PrefetchScalarGridSpec(
        num_scalar_prefetch=1,
        grid=(1,),
        in_specs=[whole(own.shape), whole(other.shape), far]
        + [whole(w.shape) for w in other_weight],
        out_specs=[whole((half, width))] * (2 * n),
        scratch_shapes=[pltpu.VMEM((n, inner, width), bf16), pltpu.SemaphoreType.DMA((n, cuts))],
    )
    return pl.pallas_call(
        body,
        grid_spec=grid_spec,
        out_shape=[jax.ShapeDtypeStruct((half, width), bf16)] * (2 * n),
        compiler_params=pltpu.CompilerParams(vmem_limit_bytes=46 * 2**20),
        cost_estimate=pl.CostEstimate(
            flops=4 * rows * inner * width * n, bytes_accessed=4 * inner * width * n, transcendentals=0
        ),
        name="spread",
    )(rank, own, other, own_weight, *other_weight)


def after(value, *others):
    return lax.optimization_barrier((value, *others))[0]


def plane_shards(checkpoint, norm_gain, query_weight, key_weight, value_weight, output_weight, block_order):
    tok_rows, width = checkpoint.shape
    block_rows = tok_rows // 2
    context_rank = lax.axis_index("cp")
    context_size = lax.axis_size("cp")
    tensor_rank = lax.axis_index("tp")
    rank = tensor_rank.astype(jnp.int32)[None]
    row_offsets = jnp.arange(block_rows, dtype=jnp.int32)
    own_blocks = lax.dynamic_slice_in_dim(block_order, 2 * context_rank, 2)
    positions = (own_blocks[:, None] * block_rows + row_offsets[None, :]).reshape(tok_rows)
    gains = norm_gain.reshape(-1, 1, width)
    CORE, X, Y = 1, 2, 4

    def tp(block, mask):
        return flip(block, "tp", mask)

    half = block_rows // 2
    own_core = tp(checkpoint, CORE)
    weights = (query_weight, key_weight, value_weight)
    begun = begin(rank, gains, 0, [checkpoint], weights, 2)
    freed = begun[2]
    begun = begin(rank, gains, 1, [own_core], weights, 2, begun)

    gathered = []
    for n in range(2):
        start = n * block_rows
        if n:
            checkpoint_later = after(checkpoint, freed)
        else:
            checkpoint_later = checkpoint
        lo = checkpoint_later[start : start + half]
        hi = checkpoint_later[start + half : start + block_rows]
        x_hi, y_lo = tp(hi, X), tp(lo, Y)
        x_lo, y_hi = tp(lo, X), tp(hi, Y)
        d_lo, d_hi = tp(y_lo, X), tp(x_hi, Y)
        pieces = [[(checkpoint, start, block_rows)], [(own_core, start, block_rows)]]
        for part in ((x_lo, x_hi), (y_lo, y_hi), (d_lo, d_hi)):
            pieces.append([(p, 0, half) for p in part])
            pieces.append([(tp(p, CORE), 0, half) for p in part])
        gathered.append(pieces)

    tables = rope_tables(positions)
    key_value = [(key_weight, True), (value_weight, False)]
    chunks, context = [], []
    for n in range(2):
        product, *sums = begun[3 * n : 3 * n + 3]
        scaled, *sums = normalise(rank, gains, 2, gathered[n][2:6], key_value, sums)
        rest, own, cosine, sine = normalise(rank, gains, 6, gathered[n][6:], key_value, sums, tables, n * block_rows)
        others = []
        for d in range(1, context_size):
            others.append(flip(own, "cp", d))
        context.append([own, *others])
        chunks.append(([scaled, rest], cosine, sine, product))
    blocks = [CORE ^ (2 * slot) for slot in range(lax.axis_size("tp") // 2)]
    *queries, a, b, c, d = project(rank, chunks, query_weight, 2, output_weight, blocks)
    other_weight = [tp(w, CORE) for w in (a, b, c, d)]

    place = context_rank.astype(jnp.int32)[None]
    pieces = [piece for pair in zip(*context) for piece in pair]
    results, normalizers = [], []
    for c in range(2):
        attended, normalizer = attend(queries[c], c, block_order, place, pieces)
        normalizers.append(normalizer[:, 0])
        partner = tp(attended, CORE)

        def deliver(slots):
            return spread(rank, slots, attended, partner, output_weight, [other_weight[s] for s in slots])

        d_lo, d_hi = deliver([3])
        d_lo, d_hi = tp(d_lo, X), tp(d_hi, Y)
        x_lo, x_hi, y_lo, y_hi = deliver([1, 2])
        s_lo, s_hi = deliver([0])
        add = lambda *terms: functools.reduce(jnp.add, [t.astype(f32) for t in terms])
        x_lo, y_hi = tp(x_lo, X), tp(y_hi, Y)
        x_hi = tp(add(x_hi, d_hi).astype(bf16), X)
        y_lo = tp(add(y_lo, d_lo).astype(bf16), Y)
        results.append(add(s_lo, x_lo, y_lo).astype(bf16))
        results.append(add(s_hi, x_hi, y_hi).astype(bf16))
    projected = jnp.concatenate(results[:2] * 2, axis=0)
    for i in (2, 3):
        projected = lax.dynamic_update_slice(projected, results[i], (i * half, 0))
    return projected, jnp.concatenate(normalizers, axis=1)


def partner_2(block, axis, stride):
    count = lax.axis_size(axis)
    route = []
    for low in range(count):
        high = low | 1 << stride
        if high != low and high < count:
            route += [(low, high), (high, low)]
    return lax.ppermute(block, axis, route)


def turn_pairs(matrix, positions, first_pair):
    pair_count = matrix.shape[-1] // 2
    pair_index = (first_pair + jnp.arange(pair_count, dtype=jnp.int32)).astype(jnp.float32)
    inverse_rates = rope_base ** (-2.0 * pair_index / HEAD_DIM)
    angles = positions.astype(jnp.float32)[:, None] * inverse_rates[None, :]
    cosine = jnp.cos(angles)[:, None, :]
    sine_part = jnp.sin(angles)[:, None, :]
    paired = matrix.reshape(matrix.shape[0], matrix.shape[1], pair_count, 2)
    former = paired[..., 0]
    latter = paired[..., 1]
    turned = jnp.stack(
        [former * cosine - latter * sine_part, former * sine_part + latter * cosine], axis=-1
    )
    return turned.reshape(matrix.shape)


def shards(
    checkpoint, norm_gain, query_weight, key_weight, value_weight, output_weight, block_order
):
    tok_rows = checkpoint.shape[0]
    block_rows = tok_rows // 2
    local_heads = query_weight.shape[1] // HEAD_DIM
    key_columns = key_weight.shape[1]
    context_rank = lax.axis_index("cp")
    tensor_rank = lax.axis_index("tp")
    row_offsets = jnp.arange(block_rows, dtype=jnp.int32)
    own_blocks = lax.dynamic_slice_in_dim(block_order, 2 * context_rank, 2)
    own_positions = (own_blocks[:, None] * block_rows + row_offsets[None, :]).reshape(tok_rows)
    gathered = lax.all_gather(checkpoint, "tp", axis=1, tiled=True)
    widened = gathered.astype(jnp.float32)
    mean_square = jnp.mean(widened * widened, axis=-1, keepdims=True)
    normed = (widened * lax.rsqrt(mean_square + norm_epsilon) * norm_gain).astype(jnp.bfloat16)
    query_features = jnp.dot(normed, query_weight, preferred_element_type=jnp.float32)
    key_features = jnp.dot(normed, key_weight, preferred_element_type=jnp.float32)
    value_features = jnp.dot(normed, value_weight, preferred_element_type=jnp.float32)
    queries = turn_pairs(
        query_features.reshape(tok_rows, local_heads, HEAD_DIM), own_positions, 0
    ).astype(jnp.bfloat16)
    sharing = lax.axis_size("tp") // KV_HEADS
    part_of_head = tensor_rank % sharing
    key_part = turn_pairs(
        key_features.reshape(tok_rows, 1, key_columns),
        own_positions,
        part_of_head * (key_columns // 2),
    )
    key_part = key_part.astype(jnp.bfloat16).reshape(tok_rows, key_columns)
    value_part = value_features.astype(jnp.bfloat16)
    own_pair = jnp.stack([key_part, value_part])
    if sharing == 2:
        partner = partner_2(own_pair, "tp", 0)
        lower_first = jnp.concatenate([own_pair, partner], axis=-1)
        upper_first = jnp.concatenate([partner, own_pair], axis=-1)
        key_value = jnp.where(part_of_head == 0, lower_first, upper_first)
    else:
        key_value = own_pair
    score_scale = 1.0 / math.sqrt(HEAD_DIM)

    def absorb(running, query_slot, key_block, key_rows, value_rows):
        query_block = own_blocks[query_slot]
        top_scores, totals, weighted = running
        query_rows = queries[query_slot * block_rows : (query_slot + 1) * block_rows]
        scores = (
            jnp.einsum("qhd,kd->qhk", query_rows, key_rows, preferred_element_type=jnp.float32)
            * score_scale
        )
        query_places = query_block * block_rows + row_offsets
        key_places = key_block * block_rows + row_offsets
        allowed = (key_places[None, :] <= query_places[:, None])[:, None, :]
        scores = jnp.where(allowed, scores, masked_score)
        old_top = top_scores[query_slot]
        new_top = jnp.maximum(old_top, jnp.max(scores, axis=-1))
        weights = jnp.where(allowed, jnp.exp(scores - new_top[..., None]), 0.0)
        shrink = jnp.exp(old_top - new_top)
        new_total = totals[query_slot] * shrink + jnp.sum(weights, axis=-1)
        new_sum = weighted[query_slot] * shrink[..., None] + jnp.einsum(
            "qhk,kd->qhd",
            weights.astype(jnp.bfloat16),
            value_rows,
            preferred_element_type=jnp.float32,
        )
        return (
            top_scores.at[query_slot].set(new_top),
            totals.at[query_slot].set(new_total),
            weighted.at[query_slot].set(new_sum),
        )

    def visit_rows(running, key_value_rows, first_row):
        block_count = key_value_rows.shape[1] // block_rows

        def one_block(block_index, current):
            rows_here = lax.dynamic_slice_in_dim(
                key_value_rows, block_index * block_rows, block_rows, 1
            )
            stored = first_row // block_rows + block_index
            key_block = lax.dynamic_index_in_dim(block_order, stored, 0, keepdims=False)
            for query_slot in range(2):
                current = absorb(current, query_slot, key_block, rows_here[0], rows_here[1])
            return current

        return lax.fori_loop(0, block_count, one_block, running)

    running = (
        jnp.full((2, block_rows, local_heads), masked_score, jnp.float32),
        jnp.zeros((2, block_rows, local_heads), jnp.float32),
        jnp.zeros((2, block_rows, local_heads, HEAD_DIM), jnp.float32),
    )
    running = visit_rows(running, key_value, context_rank * tok_rows)
    context_size = lax.axis_size("cp")

    def pass_turn(turn_index, carried):
        current, travelling = carried
        travelling = from_behind(travelling, "cp", 1)
        source = (context_rank - turn_index) % context_size
        return (visit_rows(current, travelling, source * tok_rows), travelling)

    running, _ = lax.fori_loop(1, context_size, pass_turn, (running, key_value))
    top_scores, totals, weighted = running
    attended = (
        (weighted / totals[..., None])
        .astype(jnp.bfloat16)
        .reshape(tok_rows, local_heads * HEAD_DIM)
    )
    normalizer = jnp.transpose((top_scores + jnp.log(totals)).reshape(tok_rows, local_heads))
    partial_terms = jnp.dot(attended, output_weight, preferred_element_type=jnp.float32)
    projected = lax.psum_scatter(
        partial_terms.astype(jnp.bfloat16), "tp", scatter_dimension=1, tiled=True
    )
    return (projected, normalizer)


def solution(mesh):
    around = mesh.shape["cp"]
    plane = mesh.shape["tp"] == KV_HEADS and around & (around - 1) == 0

    def body(*args):
        return plane_shards(*args)

    return jax.shard_map(
        body if plane else shards,
        mesh=mesh,
        in_specs=(
            P("cp", "tp"),
            P(),
            P(None, "tp"),
            P(None, "tp"),
            P(None, "tp"),
            P("tp", None),
            P(),
        ),
        out_specs=(P("cp", "tp"), P("tp", "cp")),
        check_vma=False,
    )
```
